128 devices in a mesh: ocn: 8 (over z, core), lon: 16 (over y, x).
Axes of the slice: x: 4, y: 4, z: 4, core: 2. Of those that a mesh axis runs over, the one named last changes fastest.
Arguments:
- ocean_state: bfloat16 [4, 12288, 128], P(None, ('ocn', 'lon')), may hold values from -6 to 6
- ice_cover: bfloat16 [12288, 128], P(('ocn', 'lon')), may hold values from 0 to 1
- ice_temp: bfloat16 [12288, 128], P(('ocn', 'lon')), may hold values from -6 to 6
- sea_mask: int32 [12288, 128], P(('ocn', 'lon')), may hold values from 0 to 1
- remap_tiles: bfloat16 [128, 640, 128, 128], P(('ocn', 'lon')), may hold values from 0 to 0.015625
- source_tile: int32 [128, 128, 5], P(('ocn', 'lon')), may hold values from 0 to 95
- send_block: int32 [128, 128, 5], P(('ocn', 'lon')), may hold values from -1 to 49, as said below
- recv_block: int32 [128, 128, 5], P(('ocn', 'lon')), may hold values from -1 to 49, as said below
- atm_state: float32 [4, 6400, 128], P(None, ('ocn', 'lon')), may hold values from -6 to 6
Outputs:
- ocean_fluxes: float32 [6, 12288, 128], P(None, ('ocn', 'lon'))
- atm_fluxes: float32 [6, 6400, 128], P(None, ('ocn', 'lon'))
The draws below stay inside these ranges and needn't reach their ends.
Inputs may be any that keep to these rules, and one draw needn't show every extreme that they name: `send_block`: -1 marks an empty slot; every slot from a device to itself is filled. recv_block[e, s, c] equals send_block[s, e, c].
All inputs are finite; a program needn't handle non-finite values.
Results may differ from the reference program's by a relative error of at most 0.0019.
Values may be sent and summed in bfloat16 or wider, within the bound.
A program may use at most 64 MiB of HBM per device.

```python
import math
import jax
import jax.numpy as jnp
from jax import lax

TILE = 128
OB_DEV = 96
AB_DEV = 50
CAP = 5
OBT = 12288
ATB = 6400
SLOTS = 640
N_OCN = 8
N_LON = 16
DEVICES = 128


def intersection_table(key):
    base = jax.random.fold_in(key, 31)
    first, second = jax.random.split(base)
    sender = jnp.arange(DEVICES, dtype=jnp.int32)[:, None, None]
    target = jnp.arange(DEVICES, dtype=jnp.int32)[None, :, None]
    rolled = jax.random.randint(first, (DEVICES, DEVICES, CAP), 0, 100)
    limit = jnp.where(target // N_LON == N_OCN - 1, 95, 35)
    filled = (rolled < limit) | (sender == target)
    blocks = jax.random.randint(second, (DEVICES, DEVICES, CAP), 0, AB_DEV)
    return jnp.where(filled, blocks, -1).astype(jnp.int32)


def source_table(key):
    base = jax.random.fold_in(key, 47)
    return jax.random.randint(base, (DEVICES, DEVICES, CAP), 0, OB_DEV).astype(jnp.int32)


def draw_send_block(key, part):
    return intersection_table(key)


def draw_recv_block(key, part):
    return intersection_table(key).transpose(1, 0, 2)


def draw_source_tile(key, part):
    return source_table(key)


def draw_sea_mask(key, part):
    base = jax.random.fold_in(key, 61)
    first, second, third = jax.random.split(base, 3)
    coastal = jax.random.randint(first, (OBT, 1), 0, 100) < 4
    sparse = jax.random.randint(second, (OBT, 1), 0, 11)
    limit = jnp.where(coastal, sparse, 3 * TILE // 4)
    cells = jax.random.randint(third, (OBT, TILE), 0, TILE)
    return (cells < limit).astype(jnp.int32)


def draw_remap_tiles(key, part):
    base = jax.random.fold_in(key, 67)
    first, second, third, fourth = jax.random.split(base, 4)
    sources = source_table(key)
    blocks = intersection_table(key)
    ocean_weak = jax.random.randint(first, (DEVICES, OB_DEV), 0, 100) < 5
    atm_weak = jax.random.randint(second, (DEVICES, AB_DEV), 0, 100) < 5
    sender = jnp.arange(DEVICES, dtype=jnp.int32)[:, None, None]
    target = jnp.arange(DEVICES, dtype=jnp.int32)[None, :, None]
    partial_slot = ocean_weak[sender, sources] | atm_weak[target, jnp.maximum(blocks, 0)] & (blocks >= 0)
    factor = jnp.exp(jax.random.uniform(third, (DEVICES, DEVICES, CAP), jnp.float32, math.log(0.004), math.log(0.04)))
    scale = jnp.where(partial_slot, factor, 1.0).reshape(DEVICES, SLOTS, 1, 1)
    values = jax.random.uniform(fourth, (DEVICES, SLOTS, TILE, TILE), jnp.float32, 0.0, 2.0 / TILE)
    return (values * scale).astype(jnp.bfloat16)


def steps_of(stream_key, shape, cuts, least, top_value):
    level = 1.0
    for dim, blocks in cuts:
        steps = jax.random.uniform(jax.random.fold_in(jax.random.fold_in(stream_key, 6), dim), (blocks,), jnp.float32, least / len(cuts), top_value / len(cuts))
        level = level * jnp.repeat(jnp.exp(steps), shape[dim] // blocks).reshape((-1,) + (1,) * (len(shape) - 1 - dim))
    return level


def bell_draw(key, extent, spread, most, cuts=(), kind=jnp.bfloat16):
    gain = steps_of(key, extent, cuts, -0.22, 0.18) if cuts else 1.0
    result = jax.random.normal(key, extent, jnp.float32) * spread * gain
    return jnp.minimum(jnp.maximum(result, -most), most).astype(kind)


def setup_inputs(seed: int = 0) -> dict:
    key_of = jax.random.split(jax.random.key(seed), 10)
    ocean_state = bell_draw(key_of[0], (4, OBT, TILE), 1.0, 6.0, ((1, 128),))
    ice_cover = jnp.clip(1.0 * jax.random.uniform(key_of[1], (OBT, TILE), jnp.float32) ** steps_of(key_of[1], (OBT, TILE), ((0, 128),), -0.2, 0.2), 0.0, 1.0).astype(jnp.bfloat16)
    ice_temp = bell_draw(key_of[2], (OBT, TILE), 1.0, 6.0, ((0, 128),))
    sea_mask = draw_sea_mask(jax.random.fold_in(key_of[9], 71), 0)
    remap_tiles = draw_remap_tiles(jax.random.fold_in(key_of[9], 71), 0)
    source_tile = draw_source_tile(jax.random.fold_in(key_of[9], 71), 0)
    send_block = draw_send_block(jax.random.fold_in(key_of[9], 71), 0)
    recv_block = draw_recv_block(jax.random.fold_in(key_of[9], 71), 0)
    atm_state = bell_draw(key_of[8], (4, ATB, TILE), 1.0, 6.0, ((1, 128),), jnp.float32)
    return {"ocean_state": ocean_state, "ice_cover": ice_cover, "ice_temp": ice_temp, "sea_mask": sea_mask, "remap_tiles": remap_tiles, "source_tile": source_tile, "send_block": send_block, "recv_block": recv_block, "atm_state": atm_state}


highest = lax.Precision.HIGHEST

def stack_fields(ocean_state, ice_cover, ice_temp, sea_mask):
    sea_frac = sea_mask.astype(jnp.bfloat16)
    fields = jnp.concatenate([ocean_state, ice_cover[None], ice_temp[None]], 0)
    return jnp.concatenate([fields * sea_frac[None], sea_frac[None]], 0)

def bulk_fluxes(gathered, atm_state):
    inverse = 1.0 / jnp.maximum(gathered[6], 0.1)
    surface_temp = gathered[0] * inverse
    current_u = gathered[1] * inverse
    current_v = gathered[2] * inverse
    salinity = gathered[3] * inverse
    ice_frac = gathered[4] * inverse
    ice_surface = gathered[5] * inverse
    slip_east = atm_state[0] - current_u
    slip_north = atm_state[1] - current_v
    wind_speed = jnp.sqrt(slip_east * slip_east + slip_north * slip_north + 0.25)
    open_water = 1.0 - ice_frac
    saturation = 0.5 * jnp.exp(0.2 * surface_temp) * (1.0 - 0.05 * salinity)
    evaporation = 0.3 * open_water * wind_speed * (saturation - atm_state[3])
    heat = 0.3 * wind_speed * (open_water * (surface_temp - atm_state[2]) + ice_frac * (ice_surface - atm_state[2])) + 2.5 * evaporation
    return jnp.stack([0.5 * open_water * wind_speed * slip_east, 0.5 * open_water * wind_speed * slip_north, 0.8 * ice_frac * wind_speed * slip_east, 0.8 * ice_frac * wind_speed * slip_north, heat, evaporation], 0)

def reference(ocean_state, ice_cover, ice_temp, sea_mask, remap_tiles, source_tile, send_block, recv_block, atm_state):
    devices = remap_tiles.shape[0]
    slots = remap_tiles.shape[1]
    stacked = stack_fields(ocean_state, ice_cover, ice_temp, sea_mask)
    per_device = stacked.reshape(7, devices, OB_DEV, TILE).transpose(1, 0, 2, 3)
    sources = source_tile.reshape(devices, slots)
    targets = send_block.reshape(devices, slots)

    def forward(item):
        fields, tiles, sources_one, targets_one = item
        picked = jnp.take(fields, sources_one, axis=1).astype(jnp.float32)
        contrib = jnp.einsum('fsi,sij->sfj', picked, tiles.astype(jnp.float32), precision=highest)
        filled = (targets_one >= 0).astype(jnp.float32)
        return (contrib * filled[:, None, None]).astype(jnp.bfloat16)
    contribs = lax.map(forward, (per_device, remap_tiles, sources, targets))
    arriving = contribs.reshape(devices, devices, CAP, 7, TILE).transpose(1, 0, 2, 3, 4).reshape(devices, slots, 7, TILE)
    atm_dev = atm_state.reshape(4, devices, AB_DEV, TILE).transpose(1, 0, 2, 3)
    incoming = recv_block.reshape(devices, slots)

    def atmosphere(item):
        received, blocks, state = item
        onehot = (blocks[None, :] == jnp.arange(AB_DEV, dtype=jnp.int32)[:, None]).astype(jnp.float32)
        gathered = jnp.einsum('bs,sfj->fbj', onehot, received.astype(jnp.float32), precision=highest)
        fluxes = bulk_fluxes(gathered, state)
        back = jnp.einsum('bs,fbj->sfj', onehot, fluxes, precision=highest).astype(jnp.bfloat16)
        return (fluxes, back)
    fluxes, backs = lax.map(atmosphere, (arriving, incoming, atm_dev))
    returning = backs.reshape(devices, devices, CAP, 6, TILE).transpose(1, 0, 2, 3, 4).reshape(devices, slots, 6, TILE)
    sea_dev = sea_mask.reshape(devices, OB_DEV, TILE)

    def ocean(item):
        received, tiles, sources_one, targets_one, sea_one = item
        filled = (targets_one >= 0).astype(jnp.float32)
        onehot = (sources_one[None, :] == jnp.arange(OB_DEV, dtype=jnp.int32)[:, None]).astype(jnp.float32) * filled[None, :]
        tiles_wide = tiles.astype(jnp.float32)
        terms = jnp.einsum('sfj,sij->sfi', received.astype(jnp.float32), tiles_wide, precision=highest)
        coverage = lax.optimization_barrier(jnp.sum(tiles_wide, axis=2))
        summed = jnp.einsum('bs,sfi->fbi', onehot, terms, precision=highest)
        cover = jnp.dot(onehot, coverage, precision=highest)
        return summed / jnp.maximum(cover, 0.1)[None] * sea_one.astype(jnp.float32)[None]
    ocean_dev = lax.map(ocean, (returning, remap_tiles, sources, targets, sea_dev))
    ocean_fluxes = ocean_dev.transpose(1, 0, 2, 3).reshape(6, devices * OB_DEV, TILE)
    atm_fluxes = fluxes.transpose(1, 0, 2, 3).reshape(6, devices * AB_DEV, TILE)
    return (ocean_fluxes, atm_fluxes)
```

```python
import jax
import jax.numpy as jnp
from jax import lax
from jax.experimental import pallas as pl
from jax.experimental.pallas import tpu as pltpu
from jax.sharding import PartitionSpec as P

MESH = pl.DeviceIdType.MESH
ABP = 56
EARLY = 3
BACK_NEAR = True
LAG = 8


def exchange_kernel(dims, ocean, ice, ice_t, sea, tiles, src, snd, rcv, atm, ocean_out, atm_out,
                    ocean_v, ice_v, icet_v, sea_v, tiles_v, src_s, rcv_s, src_v, snd_v, rcv_v, atm_v,
                    stk, send1, recv1, send2, recv2, gath, ftab, terms, summed, in_sem, tile_sem, ssem1, rsem1, ssem2, rsem2):
    n_ocn, n_lon, cap, ob, ab, nz, ny, nx = dims
    core_n = n_ocn // nz
    f32, bf16 = jnp.float32, jnp.bfloat16
    o0, l0 = lax.axis_index("ocn"), lax.axis_index("lon")
    me = o0 * n_lon + l0
    z0, c0 = o0 // core_n, lax.rem(o0, core_n)
    y0, x0 = l0 // nx, lax.rem(l0, nx)
    half = n_lon // 2
    wave_slots = n_lon * cap
    peers = n_ocn * n_lon

    def wave_offset(w):
        i = w // core_n
        dz = lax.rem(i + 2, 4) + (i // 2) * (5 - 2 * i)
        return dz, core_n - 1 - lax.rem(w, core_n)

    def wave_to(w, near=False):
        w = n_ocn - 1 - w if near else w
        dz, dc = wave_offset(w)
        return lax.rem(z0 + dz, nz) * core_n + lax.rem(c0 + dc, core_n)

    def wave_from(w, near=False):
        w = n_ocn - 1 - w if near else w
        dz, dc = wave_offset(w)
        return lax.rem(z0 - dz + nz, nz) * core_n + lax.rem(c0 - dc + core_n, core_n)

    def lon_to(i):
        dy, dx = ny - 1 - i // nx, nx - 1 - lax.rem(i, nx)
        return lax.rem(y0 + dy, ny) * nx + lax.rem(x0 + dx, nx)

    small = [(ocean, ocean_v), (ice, ice_v), (ice_t, icet_v), (sea, sea_v), (src, src_s)]
    later = [(rcv, rcv_s), (src, src_v), (snd, snd_v), (rcv, rcv_v), (atm, atm_v.at[pl.ds(0, 4 * ab)])]
    copies = [pltpu.make_async_copy(a, b, in_sem.at[i]) for i, (a, b) in enumerate(small + later)]
    for c in copies[: len(small)]:
        c.start()

    def tile_copy(w):
        rows = pl.ds(wave_to(w) * wave_slots, wave_slots)
        return pltpu.make_async_copy(tiles.at[rows], tiles_v.at[rows], tile_sem.at[w])

    def start_tiles(w, _):
        tile_copy(w).start()
        return 0

    lax.fori_loop(0, n_ocn, start_tiles, 0)
    for c in copies[len(small):]:
        c.start()

    recv1[:, 32:40, :] = jnp.zeros((peers, 8, 128), bf16)

    barrier = pltpu.get_barrier_semaphore()

    def greet(k, _):
        o = wave_to(k // n_lon)
        l = lon_to(lax.rem(k, n_lon))

        @pl.when(k != peers - 1)
        def _():
            pl.semaphore_signal(barrier, inc=1, device_id=(o, l), device_id_type=MESH)

        return 0

    lax.fori_loop(0, peers, greet, 0)

    for c in copies[: len(small)]:
        c.wait()
    sea_f = sea_v[...].astype(f32)
    for f in range(4):
        stk[:, f, :] = ocean_v[f].astype(f32) * sea_f
    stk[:, 4, :] = ice_v[...].astype(f32) * sea_f
    stk[:, 5, :] = icet_v[...].astype(f32) * sea_f
    stk[:, 6, :] = sea_f
    stk[:, 7, :] = jnp.zeros((ob, 128), f32)

    sub = lax.broadcasted_iota(jnp.int32, (8, 128), 0)

    def forward(w):
        o = wave_to(w)

        def part(h, _):
            for i in range(half):
                e = o * n_lon + lon_to(h * half + i)
                rows = [
                    jnp.dot(
                        stk[src_s[c, 0, e]].astype(bf16), tiles_v[e * cap + c], preferred_element_type=f32
                    )
                    for c in range(cap)
                ]
                for c in range(4):
                    rows[c] = jnp.where(sub == 7, pltpu.roll(rows[4], 7 - c, 0), rows[c])
                rows[4] = pltpu.roll(rows[4], 4, 0)
                for c in range(cap):
                    send1[e, 8 * c : 8 * c + 8, :] = rows[c].astype(bf16)
            return 0

        tile_copy(w).wait()
        lax.fori_loop(0, 2, part, 0)

    def push(w, buf, out, ssem, rsem, rows, near=False):
        o = wave_to(w, near)
        last = 0 if near else n_ocn - 1

        def one(j, _):
            l = lon_to(j)
            e = o * n_lon + l

            @pl.when(w * n_lon + j != last * n_lon + n_lon - 1)
            def _():
                pltpu.make_async_remote_copy(
                    buf.at[e, pl.ds(0, rows)], out.at[me, pl.ds(0, rows)], ssem, rsem.at[w], device_id=(o, l), device_id_type=MESH
                ).start()

            return 0

        lax.fori_loop(0, n_lon, one, 0)

    def forward_early(w, _):
        forward(w)
        return 0

    def push_early(w, _):
        push(w, send1, recv1, ssem1, rsem1, 36)
        return 0

    def forward_step(w, _):
        forward(w)
        push(w, send1, recv1, ssem1, rsem1, 36)
        return 0

    lax.fori_loop(0, EARLY, forward_early, 0)
    pl.semaphore_wait(barrier, peers - 1)
    lax.fori_loop(0, EARLY, push_early, 0)
    lax.fori_loop(EARLY, n_ocn, forward_step, 0)
    recv1[me] = send1[me]

    for c in copies[len(small):]:
        c.wait()

    def padded(table):
        return jnp.concatenate([table, jnp.zeros((8 - cap, peers), f32)], 0).astype(bf16)

    rcv_f = rcv_v[:, 0, :].astype(f32)
    rcv_table = padded(jnp.where(rcv_f < 0, -1000.0, rcv_f))
    src_table = padded(jnp.where(snd_v[:, 0, :] < 0, -1000.0, src_v[:, 0, :].astype(f32)))

    def onehot(table, count, o, width=None):
        rep = 1 if width is None else 8
        k = wave_slots * rep
        lanes = lax.broadcasted_iota(jnp.int32, (peers, k), 1)
        first = (lax.broadcasted_iota(jnp.int32, (peers, k), 0) - o * n_lon) * (rep * cap)
        spread = jnp.where((lanes >= first) & (lanes < first + rep * cap), 1.0, 0.0).astype(bf16)
        entries = jnp.dot(table, spread, preferred_element_type=f32)
        place = lax.rem(lax.broadcasted_iota(jnp.int32, (8, k), 1), rep * cap)
        slot = place // rep
        if width is not None:
            slot = jnp.where(lax.rem(place, rep) == 7, cap - 1, slot)
        chosen = slot == lax.broadcasted_iota(jnp.int32, (8, k), 0)
        code = jnp.sum(jnp.where(chosen, entries, 0.0), axis=0, keepdims=True)
        if width is not None:
            place = place[:1]
            field = jnp.where(lax.rem(place, rep) == 7, place // rep, lax.rem(place, rep))
            field = jnp.where(place >= rep * (cap - 1), place - (rep * (cap - 1) - 4), field)
            code = code + field.astype(f32) * float(width)
        rows = lax.broadcasted_iota(jnp.int32, (count, 1), 0).astype(f32)
        return jnp.where(rows == code, 1.0, 0.0).astype(bf16)

    def wave_wait(buf, rsem, w, rows, near=False):
        last = 0 if near else n_ocn - 1

        @pl.when(w == last)
        def _():
            part = buf.at[pl.ds(0, n_lon - 1), pl.ds(0, rows)]
            pltpu.make_async_copy(part, part, rsem.at[w]).wait()

        @pl.when(w != last)
        def _():
            part = buf.at[pl.ds(0, n_lon), pl.ds(0, rows)]
            pltpu.make_async_copy(part, part, rsem.at[w]).wait()

    gath[...] = jnp.zeros_like(gath)

    def gather_step(w, _):
        o = wave_from(w)
        hot = onehot(rcv_table, 7 * ABP, o, ABP)
        wave_wait(recv1, rsem1, w, 36)
        part = recv1[pl.ds(o * n_lon, n_lon)].reshape(n_lon * 8 * cap, 128)
        gath[...] += jnp.dot(hot, part, preferred_element_type=f32)
        return 0

    lax.fori_loop(0, n_ocn, gather_step, 0)

    atm_v[pl.ds(4 * ab, 4 * (ABP - ab)), :] = jnp.zeros((4 * (ABP - ab), 128), f32)
    g = [gath[f * ABP : (f + 1) * ABP, :] for f in range(7)]
    a = [atm_v[pl.ds(f, ABP, stride=4), :] for f in range(4)]
    inverse = 1.0 / jnp.maximum(g[6], 0.1)
    surface_temp, current_u, current_v, salinity, ice_frac, ice_surface = [g[f] * inverse for f in range(6)]
    slip_east = a[0] - current_u
    slip_north = a[1] - current_v
    wind_speed = jnp.sqrt(slip_east * slip_east + slip_north * slip_north + 0.25)
    open_water = 1.0 - ice_frac
    saturation = 0.5 * jnp.exp(0.2 * surface_temp) * (1.0 - 0.05 * salinity)
    evaporation = 0.3 * open_water * wind_speed * (saturation - a[3])
    heat = (
        0.3 * wind_speed * (open_water * (surface_temp - a[2]) + ice_frac * (ice_surface - a[2]))
        + 2.5 * evaporation
    )
    fluxes = [
        0.5 * open_water * wind_speed * slip_east,
        0.5 * open_water * wind_speed * slip_north,
        0.8 * ice_frac * wind_speed * slip_east,
        0.8 * ice_frac * wind_speed * slip_north,
        heat,
        evaporation,
    ]
    zero = jnp.zeros((ABP, 128), f32)
    for v in range(4):
        ftab[v * (ABP + 8)] = jnp.zeros((8, 128), f32)
        for r in range(8):
            if v == 0:
                value = fluxes[r] if r < 6 else zero
            else:
                value = fluxes[2 * (v - 1) + r - 6] if r >= 6 else zero
            ftab[v * (ABP + 8) + 1 : v * (ABP + 8) + 1 + ABP, r, :] = value
    for f in range(6):
        atm_out[f] = fluxes[f][:ab]

    def pack(w):
        o = wave_to(w, BACK_NEAR)

        def part(h, _):
            for i in range(half):
                e = o * n_lon + lon_to(h * half + i)

                def row(v, c):
                    return ftab[rcv_s[c, 0, e] + (v * (ABP + 8) + 1)]

                for c in range(4):
                    value = row(0, c) + row(c + 1, 4) if c < 3 else row(0, c)
                    send2[e, 8 * c : 8 * c + 8, :] = value.astype(bf16)
            return 0

        lax.fori_loop(0, 2, part, 0)

    def back_step(w, _):
        pack(w)
        push(w, send2, recv2, ssem2, rsem2, 32, BACK_NEAR)

        @pl.when(w == (0 if BACK_NEAR else n_ocn - 1))
        def _():
            recv2[me] = send2[me]

        return 0

    lax.fori_loop(0, LAG, back_step, 0)

    summed[...] = jnp.zeros_like(summed)

    def ocean_step(w, _):
        if LAG < n_ocn:

            @pl.when(w < n_ocn - LAG)
            def _():
                back_step(w + LAG, 0)

        o = wave_from(w, BACK_NEAR)
        hot = onehot(src_table, ob, o)
        wave_wait(recv2, rsem2, w, 32, BACK_NEAR)

        def part_step(p, _):
            for i in range(half):
                q = p * half + i
                s = o * n_lon + q
                block = recv2[s].astype(f32)
                v = [block[8 * c : 8 * c + 8] for c in range(4)]
                last = jnp.where(
                    sub < 2,
                    pltpu.roll(v[0], 2, 0),
                    jnp.where(sub < 4, pltpu.roll(v[1], 4, 0), pltpu.roll(v[2], 6, 0)),
                )
                for c, rows in enumerate(v + [last]):
                    lhs = jnp.where(sub == 6, 1.0, jnp.where(sub == 7, 0.0, rows)).astype(bf16)
                    term = lax.dot_general(
                        lhs, tiles_v[s * cap + c], (((1,), (1,)), ((), ())), preferred_element_type=f32
                    )
                    terms[pl.ds(q * cap + c, 8, stride=wave_slots), :] = term
            return 0

        lax.fori_loop(0, 2, part_step, 0)
        for f in range(7):
            term = terms[f * wave_slots : (f + 1) * wave_slots, :]
            hi = term.astype(bf16)
            lo = (term - hi.astype(f32)).astype(bf16)
            both = jnp.dot(hot, jnp.concatenate([hi, lo], 1), preferred_element_type=f32)
            summed[f * ob : (f + 1) * ob, :] += both[:, :128] + both[:, 128:]
        return 0

    lax.fori_loop(0, n_ocn, ocean_step, 0)
    scale = sea_v[...].astype(f32) / jnp.maximum(summed[6 * ob : 7 * ob, :], 0.1)
    for f in range(6):
        ocean_out[f] = summed[f * ob : (f + 1) * ob, :] * scale
    for buf, ssem, rows in ((send1, ssem1, 36), (send2, ssem2, 32)):
        part = buf.at[pl.ds(0, peers - 1), pl.ds(0, rows)]
        pltpu.make_async_copy(part, part, ssem).wait()


def finish_kernel(ocean_in, atm_in, ocean_out, atm_out, ocean_v, atm_v, in_sem, out_sem):
    reads = [
        pltpu.make_async_copy(ocean_in, ocean_v, in_sem.at[0]),
        pltpu.make_async_copy(atm_in, atm_v, in_sem.at[1]),
    ]
    writes = [
        pltpu.make_async_copy(ocean_v, ocean_out, out_sem.at[0]),
        pltpu.make_async_copy(atm_v, atm_out, out_sem.at[1]),
    ]
    for c in reads:
        c.start()
    for r, c in zip(reads, writes):
        r.wait()
        c.start()
    for c in writes:
        c.wait()


def shards(ocean_state, ice_cover, ice_temp, sea_mask, remap_tiles, source_tile, send_block, recv_block, atm_state):
    n_ocn, n_lon = lax.axis_size("ocn"), lax.axis_size("lon")
    peers = n_ocn * n_lon
    ob, ab = sea_mask.shape[0], atm_state.shape[1]
    slots = remap_tiles.shape[1]
    cap = slots // peers
    dims = (n_ocn, n_lon, cap, ob, ab, 4, 4, 4)
    f32, bf16, i32 = jnp.float32, jnp.bfloat16, jnp.int32

    def table(x):
        return x.transpose(2, 0, 1)

    hbm_spec = pl.BlockSpec(memory_space=pltpu.HBM)
    dma = pltpu.SemaphoreType.DMA

    def body(*refs):
        exchange_kernel(dims, *refs)

    ocean_sums, fluxes = pl.pallas_call(
        body,
        out_shape=(
            jax.ShapeDtypeStruct((6, ob, 128), f32),
            jax.ShapeDtypeStruct((6, ab, 128), f32),
        ),
        in_specs=[hbm_spec] * 9,
        out_specs=(pl.BlockSpec(memory_space=pltpu.VMEM),) * 2,
        scratch_shapes=[
            pltpu.VMEM((4, ob, 128), bf16),
            pltpu.VMEM((ob, 128), bf16),
            pltpu.VMEM((ob, 128), bf16),
            pltpu.VMEM((ob, 128), i32),
            pltpu.VMEM((slots, 128, 128), bf16),
            pltpu.SMEM((cap, 1, peers), i32),
            pltpu.SMEM((cap, 1, peers), i32),
            pltpu.VMEM((cap, 1, peers), i32),
            pltpu.VMEM((cap, 1, peers), i32),
            pltpu.VMEM((cap, 1, peers), i32),
            pltpu.VMEM((4 * ABP, 128), f32),
            pltpu.VMEM((ob, 8, 128), f32),
            pltpu.VMEM((peers, 8 * cap, 128), bf16),
            pltpu.VMEM((peers, 8 * cap, 128), bf16),
            pltpu.VMEM((peers, 32, 128), bf16),
            pltpu.VMEM((peers, 32, 128), bf16),
            pltpu.VMEM((7 * ABP, 128), f32),
            pltpu.VMEM((4 * (ABP + 8), 8, 128), f32),
            pltpu.VMEM((8 * n_lon * cap, 128), f32),
            pltpu.VMEM((7 * ob, 128), f32),
            dma((10,)),
            dma((n_ocn,)),
            dma,
            dma((n_ocn,)),
            dma,
            dma((n_ocn,)),
        ],
        compiler_params=pltpu.CompilerParams(
            collective_id=0, has_side_effects=True, vmem_limit_bytes=66300000
        ),
        name="exchange",
    )(
        ocean_state,
        ice_cover,
        ice_temp,
        sea_mask,
        remap_tiles[0],
        table(source_tile),
        table(send_block),
        table(recv_block),
        atm_state.transpose(1, 0, 2).reshape(4 * ab, 128),
    )
    return pl.pallas_call(
        finish_kernel,
        out_shape=(
            jax.ShapeDtypeStruct((6, ob, 128), f32),
            jax.ShapeDtypeStruct((6, ab, 128), f32),
        ),
        in_specs=[hbm_spec] * 2,
        out_specs=(hbm_spec,) * 2,
        scratch_shapes=[pltpu.VMEM((6, ob, 128), f32), pltpu.VMEM((6, ab, 128), f32), dma((2,)), dma((2,))],
        name="finish",
    )(ocean_sums, fluxes)


def solution(mesh):
    in_specs = (
        P(None, ("ocn", "lon"), None),
        P(("ocn", "lon"), None),
        P(("ocn", "lon"), None),
        P(("ocn", "lon"), None),
        P(("ocn", "lon"), None, None, None),
        P(("ocn", "lon"), None, None),
        P(("ocn", "lon"), None, None),
        P(("ocn", "lon"), None, None),
        P(None, ("ocn", "lon"), None),
    )
    out_specs = (P(None, ("ocn", "lon"), None), P(None, ("ocn", "lon"), None))
    return jax.shard_map(shards, mesh=mesh, in_specs=in_specs, out_specs=out_specs, check_vma=False)
```

```python
import jax
import jax.numpy as jnp
from jax import lax
from jax.experimental import pallas as pl
from jax.experimental.pallas import tpu as pltpu
from jax.sharding import PartitionSpec as P

MESH = pl.DeviceIdType.MESH
ABP = 56
EARLY = 2
BACK_NEAR = True
AHEAD = 2
LAG = 8


def slot_pairs(cap):
    slots = [(0, c) for c in range(cap)] + [(1, c) for c in range(cap)]
    return [(slots[i], slots[i + 1]) for i in range(0, 2 * cap, 2)]


def exchange_kernel(dims, ocean, ice, ice_t, sea, tiles, src, snd, rcv, atm, ocean_out, atm_out,
                    ocean_v, ice_v, icet_v, sea_v, tiles_v, src_s, rcv_s, src_v, snd_v, rcv_v, atm_v,
                    stk, send1, recv1, send2, recv2, gath, ftab, terms, summed, in_sem, tile_sem, ssem1, rsem1, ssem2, rsem2):
    n_ocn, n_lon, cap, ob, ab, nz, ny, nx = dims
    core_n = n_ocn // nz
    f32, bf16 = jnp.float32, jnp.bfloat16
    o0, l0 = lax.axis_index("ocn"), lax.axis_index("lon")
    me = o0 * n_lon + l0
    z0, c0 = o0 // core_n, lax.rem(o0, core_n)
    y0, x0 = l0 // nx, lax.rem(l0, nx)
    half = n_lon // 2
    wave_slots = n_lon * cap
    peers = n_ocn * n_lon

    def wave_offset(w):
        i = w // core_n
        dz = lax.rem(i + 2, 4) + (i // 2) * (5 - 2 * i)
        return dz, core_n - 1 - lax.rem(w, core_n)

    def wave_to(w, near=False):
        w = n_ocn - 1 - w if near else w
        dz, dc = wave_offset(w)
        return lax.rem(z0 + dz, nz) * core_n + lax.rem(c0 + dc, core_n)

    def wave_from(w, near=False):
        w = n_ocn - 1 - w if near else w
        dz, dc = wave_offset(w)
        return lax.rem(z0 - dz + nz, nz) * core_n + lax.rem(c0 - dc + core_n, core_n)

    def lon_to(i):
        dy, dx = ny - 1 - i // nx, nx - 1 - lax.rem(i, nx)
        return lax.rem(y0 + dy, ny) * nx + lax.rem(x0 + dx, nx)

    small = [(ocean, ocean_v), (ice, ice_v), (ice_t, icet_v), (sea, sea_v), (src, src_s)]
    later = [(rcv, rcv_s), (src, src_v), (snd, snd_v), (rcv, rcv_v), (atm, atm_v.at[pl.ds(0, 4 * ab)])]
    copies = [pltpu.make_async_copy(a, b, in_sem.at[i]) for i, (a, b) in enumerate(small + later)]
    for c in copies[: len(small)]:
        c.start()

    def tile_copy(w):
        rows = pl.ds(wave_to(w) * wave_slots, wave_slots)
        return pltpu.make_async_copy(tiles.at[rows], tiles_v.at[rows], tile_sem.at[w])

    for w in range(AHEAD):
        tile_copy(w).start()
    for c in copies[len(small):]:
        c.start()

    recv1[:, 32:40, :] = jnp.zeros((peers, 8, 128), bf16)

    barrier = pltpu.get_barrier_semaphore()

    def greet(k, _):
        o = wave_to(k // n_lon)
        l = lon_to(lax.rem(k, n_lon))

        @pl.when(k != peers - 1)
        def _():
            pl.semaphore_signal(barrier, inc=1, device_id=(o, l), device_id_type=MESH)

        return 0

    lax.fori_loop(0, peers, greet, 0)

    for c in copies[: len(small)]:
        c.wait()
    sea_f = sea_v[...].astype(f32)
    for f in range(4):
        stk[:, f, :] = ocean_v[f].astype(f32) * sea_f
    stk[:, 4, :] = ice_v[...].astype(f32) * sea_f
    stk[:, 5, :] = icet_v[...].astype(f32) * sea_f
    stk[:, 6, :] = sea_f
    stk[:, 7, :] = jnp.zeros((ob, 128), f32)

    sub = lax.broadcasted_iota(jnp.int32, (8, 128), 0)

    def forward(w):
        o = wave_to(w)

        def part(h, _):
            for i in range(0, half, 2):
                two = [o * n_lon + lon_to(h * half + i + d) for d in range(2)]

                def remap(p, q):
                    lhs = jnp.concatenate([stk[src_s[c, 0, two[d]]] for d, c in (p, q)], 0).astype(bf16)
                    rhs = jnp.concatenate([tiles_v[two[d] * cap + c] for d, c in (p, q)], 1)
                    both = jnp.dot(lhs, rhs, preferred_element_type=f32)
                    rows[p] = both[:8, :128]
                    rows[q] = both[8:, 128:]

                rows = {}
                for p, q in slot_pairs(cap):
                    remap(p, q)
                for d in range(2):
                    last = rows[d, cap - 1]
                    for c in range(cap - 1):
                        value = jnp.where(sub == 7, pltpu.roll(last, 7 - c, 0), rows[d, c])
                        send1[two[d], 8 * c : 8 * c + 8, :] = value.astype(bf16)
                    send1[two[d], 32:40, :] = pltpu.roll(last, 4, 0).astype(bf16)
            return 0

        @pl.when(w < n_ocn - AHEAD)
        def _():
            tile_copy(w + AHEAD).start()

        tile_copy(w).wait()
        lax.fori_loop(0, 2, part, 0)

    def push(w, buf, out, ssem, rsem, rows, near=False):
        o = wave_to(w, near)
        last = 0 if near else n_ocn - 1

        def one(j, _):
            l = lon_to(j)
            e = o * n_lon + l

            @pl.when(w * n_lon + j != last * n_lon + n_lon - 1)
            def _():
                pltpu.make_async_remote_copy(
                    buf.at[e, pl.ds(0, rows)], out.at[me, pl.ds(0, rows)], ssem, rsem.at[w], device_id=(o, l), device_id_type=MESH
                ).start()

            return 0

        lax.fori_loop(0, n_lon, one, 0)

    def forward_early(w, _):
        forward(w)
        return 0

    def push_early(w, _):
        push(w, send1, recv1, ssem1, rsem1, 36)
        return 0

    def forward_step(w, _):
        forward(w)
        push(w, send1, recv1, ssem1, rsem1, 36)
        return 0

    lax.fori_loop(0, EARLY, forward_early, 0)
    pl.semaphore_wait(barrier, peers - 1)
    lax.fori_loop(0, EARLY, push_early, 0)
    lax.fori_loop(EARLY, n_ocn, forward_step, 0)
    recv1[me] = send1[me]

    for c in copies[len(small):]:
        c.wait()

    def padded(table):
        return jnp.concatenate([table, jnp.zeros((8 - cap, peers), f32)], 0).astype(bf16)

    rcv_f = rcv_v[:, 0, :].astype(f32)
    rcv_table = padded(jnp.where(rcv_f < 0, -1000.0, rcv_f))
    src_table = padded(jnp.where(snd_v[:, 0, :] < 0, -1000.0, src_v[:, 0, :].astype(f32)))

    def onehot(table, count, o, width=None):
        rep = 1 if width is None else 8
        k = wave_slots * rep
        lanes = lax.broadcasted_iota(jnp.int32, (peers, k), 1)
        first = (lax.broadcasted_iota(jnp.int32, (peers, k), 0) - o * n_lon) * (rep * cap)
        spread = jnp.where((lanes >= first) & (lanes < first + rep * cap), 1.0, 0.0).astype(bf16)
        entries = jnp.dot(table, spread, preferred_element_type=f32)
        place = lax.rem(lax.broadcasted_iota(jnp.int32, (8, k), 1), rep * cap)
        slot = place // rep
        if width is not None:
            slot = jnp.where(lax.rem(place, rep) == 7, cap - 1, slot)
        chosen = slot == lax.broadcasted_iota(jnp.int32, (8, k), 0)
        code = jnp.sum(jnp.where(chosen, entries, 0.0), axis=0, keepdims=True)
        if width is not None:
            place = place[:1]
            field = jnp.where(lax.rem(place, rep) == 7, place // rep, lax.rem(place, rep))
            field = jnp.where(place >= rep * (cap - 1), place - (rep * (cap - 1) - 4), field)
            code = code + field.astype(f32) * float(width)
        rows = lax.broadcasted_iota(jnp.int32, (count, 1), 0).astype(f32)
        return jnp.where(rows == code, 1.0, 0.0).astype(bf16)

    def wave_wait(buf, rsem, w, rows, near=False):
        last = 0 if near else n_ocn - 1

        @pl.when(w == last)
        def _():
            part = buf.at[pl.ds(0, n_lon - 1), pl.ds(0, rows)]
            pltpu.make_async_copy(part, part, rsem.at[w]).wait()

        @pl.when(w != last)
        def _():
            part = buf.at[pl.ds(0, n_lon), pl.ds(0, rows)]
            pltpu.make_async_copy(part, part, rsem.at[w]).wait()

    gath[...] = jnp.zeros_like(gath)

    def gather_step(w, _):
        o = wave_from(w)
        hot = onehot(rcv_table, 7 * ABP, o, ABP)
        wave_wait(recv1, rsem1, w, 36)
        part = recv1[pl.ds(o * n_lon, n_lon)].reshape(n_lon * 8 * cap, 128)
        gath[...] += jnp.dot(hot, part, preferred_element_type=f32)
        return 0

    lax.fori_loop(0, n_ocn, gather_step, 0)

    atm_v[pl.ds(4 * ab, 4 * (ABP - ab)), :] = jnp.zeros((4 * (ABP - ab), 128), f32)
    g = [gath[f * ABP : (f + 1) * ABP, :] for f in range(7)]
    a = [atm_v[pl.ds(f, ABP, stride=4), :] for f in range(4)]
    inverse = 1.0 / jnp.maximum(g[6], 0.1)
    surface_temp, current_u, current_v, salinity, ice_frac, ice_surface = [g[f] * inverse for f in range(6)]
    slip_east = a[0] - current_u
    slip_north = a[1] - current_v
    wind_speed = jnp.sqrt(slip_east * slip_east + slip_north * slip_north + 0.25)
    open_water = 1.0 - ice_frac
    saturation = 0.5 * jnp.exp(0.2 * surface_temp) * (1.0 - 0.05 * salinity)
    evaporation = 0.3 * open_water * wind_speed * (saturation - a[3])
    heat = (
        0.3 * wind_speed * (open_water * (surface_temp - a[2]) + ice_frac * (ice_surface - a[2]))
        + 2.5 * evaporation
    )
    fluxes = [
        0.5 * open_water * wind_speed * slip_east,
        0.5 * open_water * wind_speed * slip_north,
        0.8 * ice_frac * wind_speed * slip_east,
        0.8 * ice_frac * wind_speed * slip_north,
        heat,
        evaporation,
    ]
    zero = jnp.zeros((ABP, 128), f32)
    for v in range(4):
        ftab[v * (ABP + 8)] = jnp.zeros((8, 128), f32)
        for r in range(8):
            if v == 0:
                value = fluxes[r] if r < 6 else zero
            else:
                value = fluxes[2 * (v - 1) + r - 6] if r >= 6 else zero
            ftab[v * (ABP + 8) + 1 : v * (ABP + 8) + 1 + ABP, r, :] = value
    for f in range(6):
        atm_out[f] = fluxes[f][:ab]

    def pack(w):
        o = wave_to(w, BACK_NEAR)

        def part(h, _):
            for i in range(half):
                e = o * n_lon + lon_to(h * half + i)

                def row(v, c):
                    return ftab[rcv_s[c, 0, e] + (v * (ABP + 8) + 1)]

                for c in range(4):
                    value = row(0, c) + row(c + 1, 4) if c < 3 else row(0, c)
                    send2[e, 8 * c : 8 * c + 8, :] = value.astype(bf16)
            return 0

        lax.fori_loop(0, 2, part, 0)

    def back_step(w, _):
        pack(w)
        push(w, send2, recv2, ssem2, rsem2, 30, BACK_NEAR)

        @pl.when(w == (0 if BACK_NEAR else n_ocn - 1))
        def _():
            recv2[me] = send2[me]

        return 0

    lax.fori_loop(0, LAG, back_step, 0)

    summed[...] = jnp.zeros_like(summed)

    def ocean_step(w, _):
        if LAG < n_ocn:

            @pl.when(w < n_ocn - LAG)
            def _():
                back_step(w + LAG, 0)

        o = wave_from(w, BACK_NEAR)
        hot = onehot(src_table, ob, o)
        wave_wait(recv2, rsem2, w, 30, BACK_NEAR)

        def part_step(p, _):
            for i in range(0, half, 2):
                place = [p * half + i + d for d in range(2)]
                base = [(o * n_lon + place[d]) * cap for d in range(2)]
                lhs = {}
                for d in range(2):
                    block = recv2[o * n_lon + place[d]].astype(f32)
                    v = [block[8 * c : 8 * c + 8] for c in range(4)]
                    last = jnp.where(
                        sub < 2,
                        pltpu.roll(v[0], 2, 0),
                        jnp.where(sub < 4, pltpu.roll(v[1], 4, 0), pltpu.roll(v[2], 6, 0)),
                    )
                    for c, rows in enumerate(v + [last]):
                        lhs[d, c] = jnp.where(sub == 6, 1.0, jnp.where(sub == 7, 0.0, rows))
                for x, y in slot_pairs(cap):
                    both = lax.dot_general(
                        jnp.concatenate([lhs[x], lhs[y]], 0).astype(bf16),
                        jnp.concatenate([tiles_v[base[d] + c] for d, c in (x, y)], 0),
                        (((1,), (1,)), ((), ())),
                        preferred_element_type=f32,
                    )
                    for (d, c), term in ((x, both[:8, :128]), (y, both[8:, 128:])):
                        terms[pl.ds(place[d] * cap + c, 8, stride=wave_slots), :] = term
            return 0

        lax.fori_loop(0, 2, part_step, 0)
        for f in range(7):
            term = terms[f * wave_slots : (f + 1) * wave_slots, :]
            hi = term.astype(bf16)
            lo = (term - hi.astype(f32)).astype(bf16)
            both = jnp.dot(hot, jnp.concatenate([hi, lo], 1), preferred_element_type=f32)
            summed[f * ob : (f + 1) * ob, :] += both[:, :128] + both[:, 128:]
        return 0

    lax.fori_loop(0, n_ocn, ocean_step, 0)
    scale = sea_v[...].astype(f32) / jnp.maximum(summed[6 * ob : 7 * ob, :], 0.1)
    for f in range(6):
        ocean_out[f] = summed[f * ob : (f + 1) * ob, :] * scale
    for buf, ssem, rows in ((send1, ssem1, 36), (send2, ssem2, 30)):
        part = buf.at[pl.ds(0, peers - 1), pl.ds(0, rows)]
        pltpu.make_async_copy(part, part, ssem).wait()


def finish_kernel(ocean_in, atm_in, ocean_out, atm_out, ocean_v, atm_v, in_sem, out_sem):
    reads = [
        pltpu.make_async_copy(ocean_in, ocean_v, in_sem.at[0]),
        pltpu.make_async_copy(atm_in, atm_v, in_sem.at[1]),
    ]
    writes = [
        pltpu.make_async_copy(ocean_v, ocean_out, out_sem.at[0]),
        pltpu.make_async_copy(atm_v, atm_out, out_sem.at[1]),
    ]
    for c in reads:
        c.start()
    for r, c in zip(reads, writes):
        r.wait()
        c.start()
    for c in writes:
        c.wait()


def shards(ocean_state, ice_cover, ice_temp, sea_mask, remap_tiles, source_tile, send_block, recv_block, atm_state):
    n_ocn, n_lon = lax.axis_size("ocn"), lax.axis_size("lon")
    peers = n_ocn * n_lon
    ob, ab = sea_mask.shape[0], atm_state.shape[1]
    slots = remap_tiles.shape[1]
    cap = slots // peers
    dims = (n_ocn, n_lon, cap, ob, ab, 4, 4, 4)
    f32, bf16, i32 = jnp.float32, jnp.bfloat16, jnp.int32

    def table(x):
        return x.transpose(2, 0, 1)

    hbm_spec = pl.BlockSpec(memory_space=pltpu.HBM)
    dma = pltpu.SemaphoreType.DMA

    def body(*refs):
        exchange_kernel(dims, *refs)

    ocean_sums, fluxes = pl.pallas_call(
        body,
        out_shape=(
            jax.ShapeDtypeStruct((6, ob, 128), f32),
            jax.ShapeDtypeStruct((6, ab, 128), f32),
        ),
        in_specs=[hbm_spec] * 9,
        out_specs=(pl.BlockSpec(memory_space=pltpu.VMEM),) * 2,
        scratch_shapes=[
            pltpu.VMEM((4, ob, 128), bf16),
            pltpu.VMEM((ob, 128), bf16),
            pltpu.VMEM((ob, 128), bf16),
            pltpu.VMEM((ob, 128), i32),
            pltpu.VMEM((slots, 128, 128), bf16),
            pltpu.SMEM((cap, 1, peers), i32),
            pltpu.SMEM((cap, 1, peers), i32),
            pltpu.VMEM((cap, 1, peers), i32),
            pltpu.VMEM((cap, 1, peers), i32),
            pltpu.VMEM((cap, 1, peers), i32),
            pltpu.VMEM((4 * ABP, 128), f32),
            pltpu.VMEM((ob, 8, 128), f32),
            pltpu.VMEM((peers, 8 * cap, 128), bf16),
            pltpu.VMEM((peers, 8 * cap, 128), bf16),
            pltpu.VMEM((peers, 32, 128), bf16),
            pltpu.VMEM((peers, 32, 128), bf16),
            pltpu.VMEM((7 * ABP, 128), f32),
            pltpu.VMEM((4 * (ABP + 8), 8, 128), f32),
            pltpu.VMEM((8 * n_lon * cap, 128), f32),
            pltpu.VMEM((7 * ob, 128), f32),
            dma((10,)),
            dma((n_ocn,)),
            dma,
            dma((n_ocn,)),
            dma,
            dma((n_ocn,)),
        ],
        compiler_params=pltpu.CompilerParams(
            collective_id=0, has_side_effects=True, vmem_limit_bytes=66300000
        ),
        name="exchange",
    )(
        ocean_state,
        ice_cover,
        ice_temp,
        sea_mask,
        remap_tiles[0],
        table(source_tile),
        table(send_block),
        table(recv_block),
        atm_state.transpose(1, 0, 2).reshape(4 * ab, 128),
    )
    return pl.pallas_call(
        finish_kernel,
        out_shape=(
            jax.ShapeDtypeStruct((6, ob, 128), f32),
            jax.ShapeDtypeStruct((6, ab, 128), f32),
        ),
        in_specs=[hbm_spec] * 2,
        out_specs=(hbm_spec,) * 2,
        scratch_shapes=[pltpu.VMEM((6, ob, 128), f32), pltpu.VMEM((6, ab, 128), f32), dma((2,)), dma((2,))],
        name="finish",
    )(ocean_sums, fluxes)


def solution(mesh):
    in_specs = (
        P(None, ("ocn", "lon"), None),
        P(("ocn", "lon"), None),
        P(("ocn", "lon"), None),
        P(("ocn", "lon"), None),
        P(("ocn", "lon"), None, None, None),
        P(("ocn", "lon"), None, None),
        P(("ocn", "lon"), None, None),
        P(("ocn", "lon"), None, None),
        P(None, ("ocn", "lon"), None),
    )
    out_specs = (P(None, ("ocn", "lon"), None), P(None, ("ocn", "lon"), None))
    return jax.shard_map(shards, mesh=mesh, in_specs=in_specs, out_specs=out_specs, check_vma=False)
```

```python
import jax
import jax.numpy as jnp
from jax import lax
from jax.experimental import pallas as pl
from jax.experimental.pallas import tpu as pltpu
from jax.sharding import PartitionSpec as P

MESH = pl.DeviceIdType.MESH
ABP = 56
EARLY = 3
BACK_NEAR = True
AHEAD = 3
LAG = 8


def slot_pairs(cap):
    slots = [(0, c) for c in range(cap)] + [(1, c) for c in range(cap)]
    return [(slots[i], slots[i + 1]) for i in range(0, 2 * cap, 2)]


def exchange_kernel(dims, ocean, ice, ice_t, sea, tiles, src, snd, rcv, atm, ocean_out, atm_out,
                    ocean_v, ice_v, icet_v, sea_v, tiles_v, src_s, rcv_s, src_v, snd_v, rcv_v, atm_v,
                    stk, send1, recv1, send2, recv2, gath, ftab, terms, summed, in_sem, tile_sem, ssem1, rsem1, ssem2, rsem2):
    n_ocn, n_lon, cap, ob, ab, nz, ny, nx = dims
    core_n = n_ocn // nz
    f32, bf16 = jnp.float32, jnp.bfloat16
    o0, l0 = lax.axis_index("ocn"), lax.axis_index("lon")
    me = o0 * n_lon + l0
    z0, c0 = o0 // core_n, lax.rem(o0, core_n)
    y0, x0 = l0 // nx, lax.rem(l0, nx)
    half = n_lon // 2
    wave_slots = n_lon * cap
    peers = n_ocn * n_lon

    def wave_offset(w):
        i = w // core_n
        dz = 3 - i
        return dz, core_n - 1 - lax.rem(w, core_n)

    def wave_to(w, near=False):
        w = n_ocn - 1 - w if near else w
        dz, dc = wave_offset(w)
        return lax.rem(z0 + dz, nz) * core_n + lax.rem(c0 + dc, core_n)

    def wave_from(w, near=False):
        w = n_ocn - 1 - w if near else w
        dz, dc = wave_offset(w)
        return lax.rem(z0 - dz + nz, nz) * core_n + lax.rem(c0 - dc + core_n, core_n)

    def lon_to(i):
        dy, dx = ny - 1 - i // nx, nx - 1 - lax.rem(i, nx)
        return lax.rem(y0 + dy, ny) * nx + lax.rem(x0 + dx, nx)

    small = [(ocean, ocean_v), (ice, ice_v), (ice_t, icet_v), (sea, sea_v), (src, src_s)]
    later = [(rcv, rcv_s), (src, src_v), (snd, snd_v), (rcv, rcv_v), (atm, atm_v.at[pl.ds(0, 4 * ab)])]
    copies = [pltpu.make_async_copy(a, b, in_sem.at[i]) for i, (a, b) in enumerate(small + later)]
    for c in copies[: len(small)]:
        c.start()

    def tile_copy(w):
        rows = pl.ds(wave_to(w) * wave_slots, wave_slots)
        return pltpu.make_async_copy(tiles.at[rows], tiles_v.at[rows], tile_sem.at[w])

    for w in range(AHEAD):
        tile_copy(w).start()
    for c in copies[len(small):]:
        c.start()

    recv1[:, 32:40, :] = jnp.zeros((peers, 8, 128), bf16)

    barrier = pltpu.get_barrier_semaphore()

    def greet(k, _):
        o = wave_to(k // n_lon)
        l = lon_to(lax.rem(k, n_lon))

        @pl.when(k != peers - 1)
        def _():
            pl.semaphore_signal(barrier, inc=1, device_id=(o, l), device_id_type=MESH)

        return 0

    lax.fori_loop(0, peers, greet, 0)

    for c in copies[: len(small)]:
        c.wait()
    sea_f = sea_v[...].astype(f32)
    for f in range(4):
        stk[:, f, :] = ocean_v[f].astype(f32) * sea_f
    stk[:, 4, :] = ice_v[...].astype(f32) * sea_f
    stk[:, 5, :] = icet_v[...].astype(f32) * sea_f
    stk[:, 6, :] = sea_f
    stk[:, 7, :] = jnp.zeros((ob, 128), f32)

    sub = lax.broadcasted_iota(jnp.int32, (8, 128), 0)

    def forward(w):
        o = wave_to(w)

        def part(h, _):
            for i in range(0, half, 2):
                two = [o * n_lon + lon_to(h * half + i + d) for d in range(2)]

                def remap(p, q):
                    lhs = jnp.concatenate([stk[src_s[c, 0, two[d]]] for d, c in (p, q)], 0).astype(bf16)
                    rhs = jnp.concatenate([tiles_v[two[d] * cap + c] for d, c in (p, q)], 1)
                    both = jnp.dot(lhs, rhs, preferred_element_type=f32)
                    rows[p] = both[:8, :128]
                    rows[q] = both[8:, 128:]

                rows = {}
                for p, q in slot_pairs(cap):
                    remap(p, q)
                for d in range(2):
                    last = rows[d, cap - 1]
                    for c in range(cap - 1):
                        value = jnp.where(sub == 7, pltpu.roll(last, 7 - c, 0), rows[d, c])
                        send1[two[d], 8 * c : 8 * c + 8, :] = value.astype(bf16)
                    send1[two[d], 32:40, :] = pltpu.roll(last, 4, 0).astype(bf16)
            return 0

        @pl.when(w < n_ocn - AHEAD)
        def _():
            tile_copy(w + AHEAD).start()

        tile_copy(w).wait()
        lax.fori_loop(0, 2, part, 0)

    def push(w, buf, out, ssem, rsem, rows, near=False):
        o = wave_to(w, near)
        last = 0 if near else n_ocn - 1

        def one(j, _):
            l = lon_to(j)
            e = o * n_lon + l

            @pl.when(w * n_lon + j != last * n_lon + n_lon - 1)
            def _():
                pltpu.make_async_remote_copy(
                    buf.at[e, pl.ds(0, rows)], out.at[me, pl.ds(0, rows)], ssem, rsem.at[w], device_id=(o, l), device_id_type=MESH
                ).start()

            return 0

        lax.fori_loop(0, n_lon, one, 0)

    def forward_early(w, _):
        forward(w)
        return 0

    def push_early(w, _):
        push(w, send1, recv1, ssem1, rsem1, 36)
        return 0

    def forward_step(w, _):
        forward(w)
        push(w, send1, recv1, ssem1, rsem1, 36)
        return 0

    lax.fori_loop(0, EARLY, forward_early, 0)
    pl.semaphore_wait(barrier, peers - 1)
    lax.fori_loop(0, EARLY, push_early, 0)
    lax.fori_loop(EARLY, n_ocn, forward_step, 0)
    recv1[me] = send1[me]

    for c in copies[len(small):]:
        c.wait()

    def padded(table):
        return jnp.concatenate([table, jnp.zeros((8 - cap, peers), f32)], 0).astype(bf16)

    rcv_f = rcv_v[:, 0, :].astype(f32)
    rcv_table = padded(jnp.where(rcv_f < 0, -1000.0, rcv_f))
    src_table = padded(jnp.where(snd_v[:, 0, :] < 0, -1000.0, src_v[:, 0, :].astype(f32)))

    def onehot(table, count, o, width=None):
        rep = 1 if width is None else 8
        k = wave_slots * rep
        lanes = lax.broadcasted_iota(jnp.int32, (peers, k), 1)
        first = (lax.broadcasted_iota(jnp.int32, (peers, k), 0) - o * n_lon) * (rep * cap)
        spread = jnp.where((lanes >= first) & (lanes < first + rep * cap), 1.0, 0.0).astype(bf16)
        entries = jnp.dot(table, spread, preferred_element_type=f32)
        place = lax.rem(lax.broadcasted_iota(jnp.int32, (8, k), 1), rep * cap)
        slot = place // rep
        if width is not None:
            slot = jnp.where(lax.rem(place, rep) == 7, cap - 1, slot)
        chosen = slot == lax.broadcasted_iota(jnp.int32, (8, k), 0)
        code = jnp.sum(jnp.where(chosen, entries, 0.0), axis=0, keepdims=True)
        if width is not None:
            place = place[:1]
            field = jnp.where(lax.rem(place, rep) == 7, place // rep, lax.rem(place, rep))
            field = jnp.where(place >= rep * (cap - 1), place - (rep * (cap - 1) - 4), field)
            code = code + field.astype(f32) * float(width)
        rows = lax.broadcasted_iota(jnp.int32, (count, 1), 0).astype(f32)
        return jnp.where(rows == code, 1.0, 0.0).astype(bf16)

    def wave_wait(buf, rsem, w, rows, near=False):
        last = 0 if near else n_ocn - 1

        @pl.when(w == last)
        def _():
            part = buf.at[pl.ds(0, n_lon - 1), pl.ds(0, rows)]
            pltpu.make_async_copy(part, part, rsem.at[w]).wait()

        @pl.when(w != last)
        def _():
            part = buf.at[pl.ds(0, n_lon), pl.ds(0, rows)]
            pltpu.make_async_copy(part, part, rsem.at[w]).wait()

    gath[...] = jnp.zeros_like(gath)
    ftab[...] = jnp.zeros_like(ftab)
    summed[...] = jnp.zeros_like(summed)

    def gather_step(w, _):
        o = wave_from(w)
        hot = onehot(rcv_table, 7 * ABP, o, ABP)
        wave_wait(recv1, rsem1, w, 36)
        part = recv1[pl.ds(o * n_lon, n_lon)].reshape(n_lon * 8 * cap, 128)
        gath[...] += jnp.dot(hot, part, preferred_element_type=f32)
        return 0

    lax.fori_loop(0, n_ocn, gather_step, 0)

    atm_v[pl.ds(4 * ab, 4 * (ABP - ab)), :] = jnp.zeros((4 * (ABP - ab), 128), f32)
    g = [gath[f * ABP : (f + 1) * ABP, :] for f in range(7)]
    a = [atm_v[pl.ds(f, ABP, stride=4), :] for f in range(4)]
    inverse = 1.0 / jnp.maximum(g[6], 0.1)
    surface_temp, current_u, current_v, salinity, ice_frac, ice_surface = [g[f] * inverse for f in range(6)]
    slip_east = a[0] - current_u
    slip_north = a[1] - current_v
    wind_speed = jnp.sqrt(slip_east * slip_east + slip_north * slip_north + 0.25)
    open_water = 1.0 - ice_frac
    saturation = 0.5 * jnp.exp(0.2 * surface_temp) * (1.0 - 0.05 * salinity)
    evaporation = 0.3 * open_water * wind_speed * (saturation - a[3])
    heat = (
        0.3 * wind_speed * (open_water * (surface_temp - a[2]) + ice_frac * (ice_surface - a[2]))
        + 2.5 * evaporation
    )
    fluxes = [
        0.5 * open_water * wind_speed * slip_east,
        0.5 * open_water * wind_speed * slip_north,
        0.8 * ice_frac * wind_speed * slip_east,
        0.8 * ice_frac * wind_speed * slip_north,
        heat,
        evaporation,
    ]
    for f in range(6):
        v = 1 + f // 2
        ftab[1 : 1 + ABP, f, :] = fluxes[f]
        ftab[v * (ABP + 8) + 1 : v * (ABP + 8) + 1 + ABP, 6 + f % 2, :] = fluxes[f]
    for f in range(6):
        atm_out[f] = fluxes[f][:ab]

    def pack(w):
        o = wave_to(w, BACK_NEAR)

        def part(h, _):
            for i in range(half):
                e = o * n_lon + lon_to(h * half + i)

                def row(v, c):
                    return ftab[rcv_s[c, 0, e] + (v * (ABP + 8) + 1)]

                for c in range(4):
                    value = row(0, c) + row(c + 1, 4) if c < 3 else row(0, c)
                    send2[e, 8 * c : 8 * c + 8, :] = value.astype(bf16)
            return 0

        lax.fori_loop(0, 2, part, 0)

    def back_step(w, _):
        pack(w)
        push(w, send2, recv2, ssem2, rsem2, 30, BACK_NEAR)

        @pl.when(w == (0 if BACK_NEAR else n_ocn - 1))
        def _():
            recv2[me] = send2[me]

        return 0

    lax.fori_loop(0, LAG, back_step, 0)


    def ocean_step(w, _):
        if LAG < n_ocn:

            @pl.when(w < n_ocn - LAG)
            def _():
                back_step(w + LAG, 0)

        o = wave_from(w, BACK_NEAR)
        hot = onehot(src_table, ob, o)
        wave_wait(recv2, rsem2, w, 30, BACK_NEAR)

        def part_step(p, _):
            for i in range(0, half, 2):
                place = [p * half + i + d for d in range(2)]
                base = [(o * n_lon + place[d]) * cap for d in range(2)]
                lhs = {}
                for d in range(2):
                    block = recv2[o * n_lon + place[d]].astype(f32)
                    v = [block[8 * c : 8 * c + 8] for c in range(4)]
                    last = jnp.where(
                        sub < 2,
                        pltpu.roll(v[0], 2, 0),
                        jnp.where(sub < 4, pltpu.roll(v[1], 4, 0), pltpu.roll(v[2], 6, 0)),
                    )
                    for c, rows in enumerate(v + [last]):
                        lhs[d, c] = jnp.where(sub == 6, 1.0, jnp.where(sub == 7, 0.0, rows))
                for x, y in slot_pairs(cap):
                    both = lax.dot_general(
                        jnp.concatenate([lhs[x], lhs[y]], 0).astype(bf16),
                        jnp.concatenate([tiles_v[base[d] + c] for d, c in (x, y)], 0),
                        (((1,), (1,)), ((), ())),
                        preferred_element_type=f32,
                    )
                    for (d, c), term in ((x, both[:8, :128]), (y, both[8:, 128:])):
                        terms[pl.ds(place[d] * cap + c, 8, stride=wave_slots), :] = term
            return 0

        lax.fori_loop(0, 2, part_step, 0)
        for f in range(7):
            term = terms[f * wave_slots : (f + 1) * wave_slots, :]
            hi = term.astype(bf16)
            lo = (term - hi.astype(f32)).astype(bf16)
            both = jnp.dot(hot, jnp.concatenate([hi, lo], 1), preferred_element_type=f32)
            summed[f * ob : (f + 1) * ob, :] += both[:, :128] + both[:, 128:]
        return 0

    lax.fori_loop(0, n_ocn, ocean_step, 0)
    scale = sea_v[...].astype(f32) / jnp.maximum(summed[6 * ob : 7 * ob, :], 0.1)
    for f in range(6):
        ocean_out[f] = summed[f * ob : (f + 1) * ob, :] * scale
    for buf, ssem, rows in ((send1, ssem1, 36), (send2, ssem2, 30)):
        part = buf.at[pl.ds(0, peers - 1), pl.ds(0, rows)]
        pltpu.make_async_copy(part, part, ssem).wait()


def finish_kernel(ocean_in, atm_in, ocean_out, atm_out, ocean_v, atm_v, in_sem, out_sem):
    reads = [
        pltpu.make_async_copy(ocean_in, ocean_v, in_sem.at[0]),
        pltpu.make_async_copy(atm_in, atm_v, in_sem.at[1]),
    ]
    writes = [
        pltpu.make_async_copy(ocean_v, ocean_out, out_sem.at[0]),
        pltpu.make_async_copy(atm_v, atm_out, out_sem.at[1]),
    ]
    for c in reads:
        c.start()
    for r, c in zip(reads, writes):
        r.wait()
        c.start()
    for c in writes:
        c.wait()


def shards(ocean_state, ice_cover, ice_temp, sea_mask, remap_tiles, source_tile, send_block, recv_block, atm_state):
    n_ocn, n_lon = lax.axis_size("ocn"), lax.axis_size("lon")
    peers = n_ocn * n_lon
    ob, ab = sea_mask.shape[0], atm_state.shape[1]
    slots = remap_tiles.shape[1]
    cap = slots // peers
    dims = (n_ocn, n_lon, cap, ob, ab, 4, 4, 4)
    f32, bf16, i32 = jnp.float32, jnp.bfloat16, jnp.int32

    def table(x):
        return x.transpose(2, 0, 1)

    hbm_spec = pl.BlockSpec(memory_space=pltpu.HBM)
    dma = pltpu.SemaphoreType.DMA

    def body(*refs):
        exchange_kernel(dims, *refs)

    ocean_sums, fluxes = pl.pallas_call(
        body,
        out_shape=(
            jax.ShapeDtypeStruct((6, ob, 128), f32),
            jax.ShapeDtypeStruct((6, ab, 128), f32),
        ),
        in_specs=[hbm_spec] * 9,
        out_specs=(pl.BlockSpec(memory_space=pltpu.VMEM),) * 2,
        scratch_shapes=[
            pltpu.VMEM((4, ob, 128), bf16),
            pltpu.VMEM((ob, 128), bf16),
            pltpu.VMEM((ob, 128), bf16),
            pltpu.VMEM((ob, 128), i32),
            pltpu.VMEM((slots, 128, 128), bf16),
            pltpu.SMEM((cap, 1, peers), i32),
            pltpu.SMEM((cap, 1, peers), i32),
            pltpu.VMEM((cap, 1, peers), i32),
            pltpu.VMEM((cap, 1, peers), i32),
            pltpu.VMEM((cap, 1, peers), i32),
            pltpu.VMEM((4 * ABP, 128), f32),
            pltpu.VMEM((ob, 8, 128), f32),
            pltpu.VMEM((peers, 8 * cap, 128), bf16),
            pltpu.VMEM((peers, 8 * cap, 128), bf16),
            pltpu.VMEM((peers, 32, 128), bf16),
            pltpu.VMEM((peers, 32, 128), bf16),
            pltpu.VMEM((7 * ABP, 128), f32),
            pltpu.VMEM((4 * (ABP + 8), 8, 128), f32),
            pltpu.VMEM((8 * n_lon * cap, 128), f32),
            pltpu.VMEM((7 * ob, 128), f32),
            dma((10,)),
            dma((n_ocn,)),
            dma,
            dma((n_ocn,)),
            dma,
            dma((n_ocn,)),
        ],
        compiler_params=pltpu.CompilerParams(
            collective_id=0, has_side_effects=True, vmem_limit_bytes=66300000
        ),
        name="exchange",
    )(
        ocean_state,
        ice_cover,
        ice_temp,
        sea_mask,
        remap_tiles[0],
        table(source_tile),
        table(send_block),
        table(recv_block),
        atm_state.transpose(1, 0, 2).reshape(4 * ab, 128),
    )
    return pl.pallas_call(
        finish_kernel,
        out_shape=(
            jax.ShapeDtypeStruct((6, ob, 128), f32),
            jax.ShapeDtypeStruct((6, ab, 128), f32),
        ),
        in_specs=[hbm_spec] * 2,
        out_specs=(hbm_spec,) * 2,
        scratch_shapes=[pltpu.VMEM((6, ob, 128), f32), pltpu.VMEM((6, ab, 128), f32), dma((2,)), dma((2,))],
        name="finish",
    )(ocean_sums, fluxes)


def solution(mesh):
    in_specs = (
        P(None, ("ocn", "lon"), None),
        P(("ocn", "lon"), None),
        P(("ocn", "lon"), None),
        P(("ocn", "lon"), None),
        P(("ocn", "lon"), None, None, None),
        P(("ocn", "lon"), None, None),
        P(("ocn", "lon"), None, None),
        P(("ocn", "lon"), None, None),
        P(None, ("ocn", "lon"), None),
    )
    out_specs = (P(None, ("ocn", "lon"), None), P(None, ("ocn", "lon"), None))
    return jax.shard_map(shards, mesh=mesh, in_specs=in_specs, out_specs=out_specs, check_vma=False)
```

```python
import jax
import jax.numpy as jnp
from jax import lax
from jax.experimental import pallas as pl
from jax.experimental.pallas import tpu as pltpu
from jax.sharding import PartitionSpec as P

MESH = pl.DeviceIdType.MESH
ABP = 56
EARLY = 4
BACK_NEAR = True
AHEAD = 3
LAG = 8


def slot_pairs(cap):
    slots = [(0, c) for c in range(cap)] + [(1, c) for c in range(cap)]
    return [(slots[i], slots[i + 1]) for i in range(0, 2 * cap, 2)]


def exchange_kernel(dims, ocean, ice, ice_t, sea, tiles, src, snd, rcv, atm, ocean_out, atm_out,
                    ocean_v, ice_v, icet_v, sea_v, tiles_v, src_s, rcv_s, src_v, snd_v, rcv_v, atm_v,
                    stk, send1, recv1, send2, recv2, gath, ftab, terms, summed, in_sem, tile_sem, ssem1, rsem1, ssem2, rsem2):
    n_ocn, n_lon, cap, ob, ab, nz, ny, nx = dims
    core_n = n_ocn // nz
    f32, bf16 = jnp.float32, jnp.bfloat16
    o0, l0 = lax.axis_index("ocn"), lax.axis_index("lon")
    me = o0 * n_lon + l0
    z0, c0 = o0 // core_n, lax.rem(o0, core_n)
    y0, x0 = l0 // nx, lax.rem(l0, nx)
    half = n_lon // 2
    wave_slots = n_lon * cap
    peers = n_ocn * n_lon

    def wave_offset(w):
        i = w // core_n
        dz = 3 - i
        return dz, core_n - 1 - lax.rem(w, core_n)

    def wave_to(w, near=False):
        w = n_ocn - 1 - w if near else w
        dz, dc = wave_offset(w)
        return lax.rem(z0 + dz, nz) * core_n + lax.rem(c0 + dc, core_n)

    def wave_from(w, near=False):
        w = n_ocn - 1 - w if near else w
        dz, dc = wave_offset(w)
        return lax.rem(z0 - dz + nz, nz) * core_n + lax.rem(c0 - dc + core_n, core_n)

    def lon_to(i):
        dy, dx = ny - 1 - i // nx, nx - 1 - lax.rem(i, nx)
        return lax.rem(y0 + dy, ny) * nx + lax.rem(x0 + dx, nx)

    small = [(ocean, ocean_v), (ice, ice_v), (ice_t, icet_v), (sea, sea_v), (src, src_s)]
    later = [(rcv, rcv_s), (src, src_v), (snd, snd_v), (rcv, rcv_v), (atm, atm_v.at[pl.ds(0, 4 * ab)])]
    copies = [pltpu.make_async_copy(a, b, in_sem.at[i]) for i, (a, b) in enumerate(small + later)]
    for c in copies[: len(small)]:
        c.start()

    def tile_copy(w):
        rows = pl.ds(wave_to(w) * wave_slots, wave_slots)
        return pltpu.make_async_copy(tiles.at[rows], tiles_v.at[rows], tile_sem.at[w])

    for w in range(AHEAD):
        tile_copy(w).start()
    for c in copies[len(small):]:
        c.start()

    recv1[:, 32:40, :] = jnp.zeros((peers, 8, 128), bf16)

    barrier = pltpu.get_barrier_semaphore()

    def greet(k, _):
        o = wave_to(k // n_lon)
        l = lon_to(lax.rem(k, n_lon))

        @pl.when(k != peers - 1)
        def _():
            pl.semaphore_signal(barrier, inc=1, device_id=(o, l), device_id_type=MESH)

        return 0

    lax.fori_loop(0, peers, greet, 0)

    for c in copies[: len(small)]:
        c.wait()
    sea_f = sea_v[...].astype(f32)
    for f in range(4):
        stk[:, f, :] = ocean_v[f].astype(f32) * sea_f
    stk[:, 4, :] = ice_v[...].astype(f32) * sea_f
    stk[:, 5, :] = icet_v[...].astype(f32) * sea_f
    stk[:, 6, :] = sea_f
    stk[:, 7, :] = jnp.zeros((ob, 128), f32)

    sub = lax.broadcasted_iota(jnp.int32, (8, 128), 0)

    def forward(w):
        o = wave_to(w)

        def part(h, _):
            for i in range(0, half, 2):
                two = [o * n_lon + lon_to(h * half + i + d) for d in range(2)]

                def remap(p, q):
                    lhs = jnp.concatenate([stk[src_s[c, 0, two[d]]] for d, c in (p, q)], 0).astype(bf16)
                    rhs = jnp.concatenate([tiles_v[two[d] * cap + c] for d, c in (p, q)], 1)
                    both = jnp.dot(lhs, rhs, preferred_element_type=f32)
                    rows[p] = both[:8, :128]
                    rows[q] = both[8:, 128:]

                rows = {}
                for p, q in slot_pairs(cap):
                    remap(p, q)
                for d in range(2):
                    last = rows[d, cap - 1]
                    for c in range(cap - 1):
                        value = jnp.where(sub == 7, pltpu.roll(last, 7 - c, 0), rows[d, c])
                        send1[two[d], 8 * c : 8 * c + 8, :] = value.astype(bf16)
                    send1[two[d], 32:40, :] = pltpu.roll(last, 4, 0).astype(bf16)
            return 0

        @pl.when(w < n_ocn - AHEAD)
        def _():
            tile_copy(w + AHEAD).start()

        tile_copy(w).wait()
        lax.fori_loop(0, 2, part, 0)

    def push(w, buf, out, ssem, rsem, rows, near=False):
        o = wave_to(w, near)
        last = 0 if near else n_ocn - 1

        def one(j, _):
            l = lon_to(j)
            e = o * n_lon + l

            @pl.when(w * n_lon + j != last * n_lon + n_lon - 1)
            def _():
                pltpu.make_async_remote_copy(
                    buf.at[e, pl.ds(0, rows)], out.at[me, pl.ds(0, rows)], ssem, rsem.at[w], device_id=(o, l), device_id_type=MESH
                ).start()

            return 0

        lax.fori_loop(0, n_lon, one, 0)

    def forward_early(w, _):
        forward(w)
        return 0

    def push_early(w, _):
        push(w, send1, recv1, ssem1, rsem1, 36)
        return 0

    def forward_step(w, _):
        forward(w)
        push(w, send1, recv1, ssem1, rsem1, 36)
        return 0

    lax.fori_loop(0, EARLY, forward_early, 0)
    pl.semaphore_wait(barrier, peers - 1)
    lax.fori_loop(0, EARLY, push_early, 0)
    lax.fori_loop(EARLY, n_ocn, forward_step, 0)
    recv1[me] = send1[me]

    for c in copies[len(small):]:
        c.wait()

    def padded(table):
        return jnp.concatenate([table, jnp.zeros((8 - cap, peers), f32)], 0).astype(bf16)

    rcv_f = rcv_v[:, 0, :].astype(f32)
    rcv_table = padded(jnp.where(rcv_f < 0, -1000.0, rcv_f))
    src_table = padded(jnp.where(snd_v[:, 0, :] < 0, -1000.0, src_v[:, 0, :].astype(f32)))

    def onehot(table, count, o, width=None):
        rep = 1 if width is None else 8
        k = wave_slots * rep
        lanes = lax.broadcasted_iota(jnp.int32, (peers, k), 1)
        first = (lax.broadcasted_iota(jnp.int32, (peers, k), 0) - o * n_lon) * (rep * cap)
        spread = jnp.where((lanes >= first) & (lanes < first + rep * cap), 1.0, 0.0).astype(bf16)
        entries = jnp.dot(table, spread, preferred_element_type=f32)
        place = lax.rem(lax.broadcasted_iota(jnp.int32, (8, k), 1), rep * cap)
        slot = place // rep
        if width is not None:
            slot = jnp.where(lax.rem(place, rep) == 7, cap - 1, slot)
        chosen = slot == lax.broadcasted_iota(jnp.int32, (8, k), 0)
        code = jnp.sum(jnp.where(chosen, entries, 0.0), axis=0, keepdims=True)
        if width is not None:
            place = place[:1]
            field = jnp.where(lax.rem(place, rep) == 7, place // rep, lax.rem(place, rep))
            field = jnp.where(place >= rep * (cap - 1), place - (rep * (cap - 1) - 4), field)
            code = code + field.astype(f32) * float(width)
        rows = lax.broadcasted_iota(jnp.int32, (count, 1), 0).astype(f32)
        return jnp.where(rows == code, 1.0, 0.0).astype(bf16)

    def wave_wait(buf, rsem, w, rows, near=False):
        last = 0 if near else n_ocn - 1

        @pl.when(w == last)
        def _():
            part = buf.at[pl.ds(0, n_lon - 1), pl.ds(0, rows)]
            pltpu.make_async_copy(part, part, rsem.at[w]).wait()

        @pl.when(w != last)
        def _():
            part = buf.at[pl.ds(0, n_lon), pl.ds(0, rows)]
            pltpu.make_async_copy(part, part, rsem.at[w]).wait()

    gath[...] = jnp.zeros_like(gath)
    ftab[...] = jnp.zeros_like(ftab)
    summed[...] = jnp.zeros_like(summed)

    def gather_step(w, _):
        o = wave_from(w)
        hot = onehot(rcv_table, 7 * ABP, o, ABP)
        wave_wait(recv1, rsem1, w, 36)
        part = recv1[pl.ds(o * n_lon, n_lon)].reshape(n_lon * 8 * cap, 128)
        gath[...] += jnp.dot(hot, part, preferred_element_type=f32)
        return 0

    lax.fori_loop(0, n_ocn, gather_step, 0)

    atm_v[pl.ds(4 * ab, 4 * (ABP - ab)), :] = jnp.zeros((4 * (ABP - ab), 128), f32)
    g = [gath[f * ABP : (f + 1) * ABP, :] for f in range(7)]
    a = [atm_v[pl.ds(f, ABP, stride=4), :] for f in range(4)]
    inverse = 1.0 / jnp.maximum(g[6], 0.1)
    surface_temp, current_u, current_v, salinity, ice_frac, ice_surface = [g[f] * inverse for f in range(6)]
    slip_east = a[0] - current_u
    slip_north = a[1] - current_v
    wind_speed = jnp.sqrt(slip_east * slip_east + slip_north * slip_north + 0.25)
    open_water = 1.0 - ice_frac
    saturation = 0.5 * jnp.exp(0.2 * surface_temp) * (1.0 - 0.05 * salinity)
    evaporation = 0.3 * open_water * wind_speed * (saturation - a[3])
    heat = (
        0.3 * wind_speed * (open_water * (surface_temp - a[2]) + ice_frac * (ice_surface - a[2]))
        + 2.5 * evaporation
    )
    fluxes = [
        0.5 * open_water * wind_speed * slip_east,
        0.5 * open_water * wind_speed * slip_north,
        0.8 * ice_frac * wind_speed * slip_east,
        0.8 * ice_frac * wind_speed * slip_north,
        heat,
        evaporation,
    ]
    for f in range(6):
        v = 1 + f // 2
        ftab[1 : 1 + ABP, f, :] = fluxes[f]
        ftab[v * (ABP + 8) + 1 : v * (ABP + 8) + 1 + ABP, 6 + f % 2, :] = fluxes[f]
    for f in range(6):
        atm_out[f] = fluxes[f][:ab]

    def pack(w):
        o = wave_to(w, BACK_NEAR)

        def part(h, _):
            for i in range(half):
                e = o * n_lon + lon_to(h * half + i)

                def row(v, c):
                    return ftab[rcv_s[c, 0, e] + (v * (ABP + 8) + 1)]

                for c in range(4):
                    value = row(0, c) + row(c + 1, 4) if c < 3 else row(0, c)
                    send2[e, 8 * c : 8 * c + 8, :] = value.astype(bf16)
            return 0

        lax.fori_loop(0, 2, part, 0)

    def back_step(w, _):
        pack(w)
        push(w, send2, recv2, ssem2, rsem2, 30, BACK_NEAR)

        @pl.when(w == (0 if BACK_NEAR else n_ocn - 1))
        def _():
            recv2[me] = send2[me]

        return 0

    lax.fori_loop(0, LAG, back_step, 0)


    def ocean_step(w, _):
        if LAG < n_ocn:

            @pl.when(w < n_ocn - LAG)
            def _():
                back_step(w + LAG, 0)

        o = wave_from(w, BACK_NEAR)
        hot = onehot(src_table, ob, o)
        wave_wait(recv2, rsem2, w, 30, BACK_NEAR)

        def part_step(p, _):
            for i in range(0, half, 2):
                place = [p * half + i + d for d in range(2)]
                base = [(o * n_lon + place[d]) * cap for d in range(2)]
                lhs = {}
                for d in range(2):
                    block = recv2[o * n_lon + place[d]].astype(f32)
                    v = [block[8 * c : 8 * c + 8] for c in range(4)]
                    last = jnp.where(
                        sub < 2,
                        pltpu.roll(v[0], 2, 0),
                        jnp.where(sub < 4, pltpu.roll(v[1], 4, 0), pltpu.roll(v[2], 6, 0)),
                    )
                    for c, rows in enumerate(v + [last]):
                        lhs[d, c] = jnp.where(sub == 6, 1.0, jnp.where(sub == 7, 0.0, rows))
                for x, y in slot_pairs(cap):
                    both = lax.dot_general(
                        jnp.concatenate([lhs[x], lhs[y]], 0).astype(bf16),
                        jnp.concatenate([tiles_v[base[d] + c] for d, c in (x, y)], 0),
                        (((1,), (1,)), ((), ())),
                        preferred_element_type=f32,
                    )
                    for (d, c), term in ((x, both[:8, :128]), (y, both[8:, 128:])):
                        terms[pl.ds(place[d] * cap + c, 8, stride=wave_slots), :] = term
            return 0

        lax.fori_loop(0, 2, part_step, 0)
        for f in range(7):
            term = terms[f * wave_slots : (f + 1) * wave_slots, :]
            hi = term.astype(bf16)
            lo = (term - hi.astype(f32)).astype(bf16)
            both = jnp.dot(hot, jnp.concatenate([hi, lo], 1), preferred_element_type=f32)
            summed[f * ob : (f + 1) * ob, :] += both[:, :128] + both[:, 128:]
        return 0

    lax.fori_loop(0, n_ocn, ocean_step, 0)
    scale = sea_v[...].astype(f32) / jnp.maximum(summed[6 * ob : 7 * ob, :], 0.1)
    for f in range(6):
        ocean_out[f] = summed[f * ob : (f + 1) * ob, :] * scale
    for buf, ssem, rows in ((send1, ssem1, 36), (send2, ssem2, 30)):
        part = buf.at[pl.ds(0, peers - 1), pl.ds(0, rows)]
        pltpu.make_async_copy(part, part, ssem).wait()


def finish_kernel(ocean_in, atm_in, ocean_out, atm_out, ocean_v, atm_v, in_sem, out_sem):
    reads = [
        pltpu.make_async_copy(ocean_in, ocean_v, in_sem.at[0]),
        pltpu.make_async_copy(atm_in, atm_v, in_sem.at[1]),
    ]
    writes = [
        pltpu.make_async_copy(ocean_v, ocean_out, out_sem.at[0]),
        pltpu.make_async_copy(atm_v, atm_out, out_sem.at[1]),
    ]
    for c in reads:
        c.start()
    for r, c in zip(reads, writes):
        r.wait()
        c.start()
    for c in writes:
        c.wait()


def shards(ocean_state, ice_cover, ice_temp, sea_mask, remap_tiles, source_tile, send_block, recv_block, atm_state):
    n_ocn, n_lon = lax.axis_size("ocn"), lax.axis_size("lon")
    peers = n_ocn * n_lon
    ob, ab = sea_mask.shape[0], atm_state.shape[1]
    slots = remap_tiles.shape[1]
    cap = slots // peers
    dims = (n_ocn, n_lon, cap, ob, ab, 4, 4, 4)
    f32, bf16, i32 = jnp.float32, jnp.bfloat16, jnp.int32

    def table(x):
        return x.transpose(2, 0, 1)

    hbm_spec = pl.BlockSpec(memory_space=pltpu.HBM)
    dma = pltpu.SemaphoreType.DMA

    def body(*refs):
        exchange_kernel(dims, *refs)

    ocean_sums, fluxes = pl.pallas_call(
        body,
        out_shape=(
            jax.ShapeDtypeStruct((6, ob, 128), f32),
            jax.ShapeDtypeStruct((6, ab, 128), f32),
        ),
        in_specs=[hbm_spec] * 9,
        out_specs=(pl.BlockSpec(memory_space=pltpu.VMEM),) * 2,
        scratch_shapes=[
            pltpu.VMEM((4, ob, 128), bf16),
            pltpu.VMEM((ob, 128), bf16),
            pltpu.VMEM((ob, 128), bf16),
            pltpu.VMEM((ob, 128), i32),
            pltpu.VMEM((slots, 128, 128), bf16),
            pltpu.SMEM((cap, 1, peers), i32),
            pltpu.SMEM((cap, 1, peers), i32),
            pltpu.VMEM((cap, 1, peers), i32),
            pltpu.VMEM((cap, 1, peers), i32),
            pltpu.VMEM((cap, 1, peers), i32),
            pltpu.VMEM((4 * ABP, 128), f32),
            pltpu.VMEM((ob, 8, 128), f32),
            pltpu.VMEM((peers, 8 * cap, 128), bf16),
            pltpu.VMEM((peers, 8 * cap, 128), bf16),
            pltpu.VMEM((peers, 32, 128), bf16),
            pltpu.VMEM((peers, 32, 128), bf16),
            pltpu.VMEM((7 * ABP, 128), f32),
            pltpu.VMEM((4 * (ABP + 8), 8, 128), f32),
            pltpu.VMEM((8 * n_lon * cap, 128), f32),
            pltpu.VMEM((7 * ob, 128), f32),
            dma((10,)),
            dma((n_ocn,)),
            dma,
            dma((n_ocn,)),
            dma,
            dma((n_ocn,)),
        ],
        compiler_params=pltpu.CompilerParams(
            collective_id=0, has_side_effects=True, vmem_limit_bytes=66300000
        ),
        name="exchange",
    )(
        ocean_state,
        ice_cover,
        ice_temp,
        sea_mask,
        remap_tiles[0],
        table(source_tile),
        table(send_block),
        table(recv_block),
        atm_state.transpose(1, 0, 2).reshape(4 * ab, 128),
    )
    return pl.pallas_call(
        finish_kernel,
        out_shape=(
            jax.ShapeDtypeStruct((6, ob, 128), f32),
            jax.ShapeDtypeStruct((6, ab, 128), f32),
        ),
        in_specs=[hbm_spec] * 2,
        out_specs=(hbm_spec,) * 2,
        scratch_shapes=[pltpu.VMEM((6, ob, 128), f32), pltpu.VMEM((6, ab, 128), f32), dma((2,)), dma((2,))],
        name="finish",
    )(ocean_sums, fluxes)


def solution(mesh):
    in_specs = (
        P(None, ("ocn", "lon"), None),
        P(("ocn", "lon"), None),
        P(("ocn", "lon"), None),
        P(("ocn", "lon"), None),
        P(("ocn", "lon"), None, None, None),
        P(("ocn", "lon"), None, None),
        P(("ocn", "lon"), None, None),
        P(("ocn", "lon"), None, None),
        P(None, ("ocn", "lon"), None),
    )
    out_specs = (P(None, ("ocn", "lon"), None), P(None, ("ocn", "lon"), None))
    return jax.shard_map(shards, mesh=mesh, in_specs=in_specs, out_specs=out_specs, check_vma=False)
```
